32 devices in a mesh: rows: 8 (over z, x), grp: 4 (over y, core).
Axes of the slice: x: 2, y: 2, z: 4, core: 2. Of those that a mesh axis runs over, the one named last changes fastest.
Arguments:
- user_features: bfloat16 [4, 2048, 256], P('grp', 'rows'), may hold values from -72 to 72
- w_first: bfloat16 [256, 256], replicated, may hold values from -0.375 to 0.375
- w_second: bfloat16 [256, 256], replicated, may hold values from -0.375 to 0.375
- item_embed: bfloat16 [4, 2048, 256], P('grp', 'rows'), may hold values from -27 to 27
- example_weight: float32 [4, 2048], P('grp', 'rows'), may hold values from 0.02 to 0.2
- positive: int32 [4, 2048], P('grp', 'rows'), may hold values from 0 to 2047
- item_owner: int32 [4, 2048, 1], P('grp', 'rows'), may hold values from 0 to 7; in each aligned block of 256 rows (0 to 255, 256 to 511, ..., all dimensions but the last counted through in order) at most 128 rows name the same one
- item_row: int32 [4, 2048], P('grp', 'rows'), may hold values from 0 to 4095
Outputs:
- grad_first: float32 [256, 256], replicated
- grad_second: float32 [256, 256], replicated
- grad_table: float32 [32768, 256], P('rows', 'grp')
The draws below stay inside these ranges and needn't reach their ends.
Inputs may be any that keep to these rules, and one draw needn't show every extreme that they name: `item_owner`: within the rows of one device (aligned blocks of 256 pairs of a group) no owner is named by more than 128 pairs, a bound that some block reaches.
All inputs are finite; a program needn't handle non-finite values.
Results may differ from the reference program's by a relative error of at most 0.0023.
The reference program's roundings to bfloat16 on the way count: a program that leaves them out, or rounds other values in their place, can miss the bound.
Values may be sent and summed in bfloat16 or wider, within the bound.
A program may use at most 128 MiB of HBM per device.

```python
import math
import jax
import jax.numpy as jnp
import numpy as np
from jax import lax

D = 256
DIN = 256
DH = 256
BATCH_DEV = 256
ITEMS_DEV = 4096
GU = 2048
CAP = 128
N_ROWS = 8
N_GRP = 4


def draw_user_features(key, part):
    first_key = jax.random.fold_in(jax.random.fold_in(key, 11), 0)
    values = jnp.clip(jax.random.normal(first_key, (N_GRP, GU, DIN), jnp.float32), -6.0, 6.0)
    return values.astype(jnp.bfloat16)


def draw_item_embed(key, part):
    first_key = jax.random.fold_in(jax.random.fold_in(key, 23), 0)
    values = 0.15 * jnp.clip(jax.random.normal(first_key, (N_GRP, GU, D), jnp.float32), -6.0, 6.0)
    return values.astype(jnp.bfloat16)


def with_ends(entries, own_key, least, top_value):
    dims = entries.shape
    place = [jax.random.randint(jax.random.fold_in(own_key, axis), (), 0, dims[axis]) for axis in range(len(dims))]
    entries = entries.at[tuple(place)].set(least)
    longest = dims.index(max(dims))
    place[longest] = (place[longest] + 1) % dims[longest]
    return entries.at[tuple(place)].set(top_value)


def shard_levels(rng, dims, shards, low, largest):
    gain = 1.0
    for axis_at, shards_of in shards:
        draws = jax.random.uniform(jax.random.fold_in(jax.random.fold_in(rng, 6), axis_at), (shards_of,), jnp.float32, low / len(shards), largest / len(shards))
        gain = gain * jnp.repeat(jnp.exp(draws), dims[axis_at] // shards_of).reshape((-1,) + (1,) * (len(dims) - 1 - axis_at))
    return gain


def cumulative_ranks(number_of, slope):
    loads = [(1 << 20) // math.isqrt(standing ** slope) + 1 for standing in range(1, number_of + 1)]
    width = 1 + sum(loads) // (1 << 30)
    return np.cumsum(np.array([max(1, weight // width) for weight in loads]))


def ranked_ids(own_key, extent, amount, lean):
    listing = cumulative_ranks(amount, lean)
    pick = jax.random.randint(jax.random.fold_in(own_key, 1), extent, 0, int(listing[amount - 1]))
    standing = jnp.searchsorted(jnp.asarray(listing, jnp.int32), pick, side="right")
    return jax.random.permutation(jax.random.fold_in(own_key, 2), amount)[standing].astype(jnp.int32)


def assign_block(rng, own, number, rows, count, top, limit, skew):
    ranking = jax.random.permutation(rng, count)
    packed, common = shares(count, rows * top, limit, skew, True), shares(count, rows * top, limit, skew, False)
    places = jnp.arange(count)

    def named(tallies, rotation):
        used = int((tallies > 0).sum())
        fixed = max(1, used // 4)
        passed = fixed + (places - fixed + rotation * (used - fixed)) % max(1, count - fixed)
        return jnp.zeros((count,), jnp.int32).at[ranking[jnp.where(places < fixed, places, passed)]].set(jnp.asarray(tallies, jnp.int32))

    tallies = jnp.where(number % 4 == 0, named(packed, number // 4), named(common, number - number // 4 - 1))
    mixed = jax.random.permutation(jax.random.fold_in(own, 3), count)
    donor, sink = mixed[0:count // 2 * 2:2], mixed[1:count // 2 * 2:2]
    room = jnp.minimum(tallies[donor] - 1, limit - tallies[sink]) // 2
    room = jnp.where((donor == ranking[0]) | (sink == ranking[0]) | (tallies[sink] == 0), 0, jnp.maximum(room, 0))
    passed = jax.random.randint(jax.random.fold_in(own, 4), (count // 2,), 0, 1 << 20) % (room + 1)
    tallies = tallies.at[donor].add(-passed).at[sink].add(passed)
    labels = jnp.searchsorted(jnp.cumsum(tallies), jnp.arange(rows * top), side="right").astype(jnp.int32)
    grid = labels.reshape(top, rows).T
    grid = grid[jax.random.permutation(jax.random.fold_in(own, 1), rows)]
    rotation = jax.random.randint(jax.random.fold_in(own, 2), (rows, 1), 0, top)
    return jnp.take_along_axis(grid, (jnp.arange(top)[None, :] + rotation) % top, axis=1)


def shares(amount, total, reach, skew, full):
    portions = [(1 << 20) // math.isqrt(grade ** skew) + 1 for grade in range(1, amount + 1)]
    largest = reach if full else min(reach, max(-(-total // amount), total * portions[0] // sum(portions)))
    least = 1 if total - largest >= amount - 1 else 0
    counts, surplus = [largest] + [least] * (amount - 1), total - largest - least * (amount - 1)
    while surplus > 0:
        candidates = [i for i in range(1, amount) if counts[i] < largest] or [i for i in range(1, amount) if counts[i] < reach]
        pool, remaining = sum([portions[i] for i in candidates]), surplus
        for i in candidates:
            more = min(reach - counts[i], max(1, remaining * portions[i] // pool), surplus)
            counts[i] = counts[i] + more
            surplus = surplus - more
    return np.array(counts)


def centred(rng, dims, scale, reach, held_as=jnp.bfloat16):
    array = scale * jax.random.normal(rng, dims, jnp.float32)
    return jnp.clip(array, min=-reach, max=reach).astype(held_as)


def setup_inputs(seed: int = 0) -> dict:
    key_list = jax.random.split(jax.random.key(seed), 9)
    user_features = draw_user_features(jax.random.fold_in(key_list[8], 71), 0)
    w_first = centred(key_list[1], (DIN, DH), DIN ** -0.5, 0.375)
    w_second = centred(key_list[2], (DH, D), DH ** -0.5, 0.375)
    item_embed = draw_item_embed(jax.random.fold_in(key_list[8], 71), 0)
    example_weight = jnp.clip(jnp.exp(math.log(0.2) - 2.3025851 * jax.random.uniform(key_list[4], (N_GRP, GU), jnp.float32) ** shard_levels(key_list[4], (N_GRP, GU), ((0, 4), (1, 8)), -0.2, 0.2)), 0.02, 0.2)
    positive = with_ends(jax.random.randint(key_list[5], (N_GRP, GU), 0, GU), jax.random.fold_in(key_list[5], 1), 0, GU - 1).astype(jnp.int32)
    item_owner_keys = jax.random.split(jax.random.fold_in(key_list[6], 1), N_GRP * GU // BATCH_DEV)
    item_owner_turns = jax.random.permutation(jax.random.fold_in(key_list[6], 3), N_GRP * GU // BATCH_DEV)
    item_owner = jax.vmap(lambda own, number: assign_block(jax.random.fold_in(key_list[6], 2), own, number, BATCH_DEV, N_ROWS, 1, CAP, 2))(item_owner_keys, item_owner_turns).reshape((N_GRP, GU, 1))
    item_row = with_ends(ranked_ids(key_list[7], (N_GRP, GU), ITEMS_DEV, 2), jax.random.fold_in(key_list[7], 3), 0, ITEMS_DEV - 1).astype(jnp.int32)
    return dict(user_features=user_features, w_first=w_first, w_second=w_second, item_embed=item_embed, example_weight=example_weight, positive=positive, item_owner=item_owner, item_row=item_row)


def reference(user_features, w_first, w_second, item_embed, example_weight, positive, item_owner, item_row):
    group_users = user_features.shape[1]
    row_block = math.gcd(group_users, 1024)
    num_blocks = group_users // row_block

    def one_group(inputs):
        features, group_items, weights, targets = inputs
        pre_act = jnp.dot(features, w_first, preferred_element_type=jnp.float32)
        hidden = jax.nn.silu(pre_act).astype(jnp.bfloat16)
        user_vecs = jnp.dot(hidden, w_second, preferred_element_type=jnp.float32).astype(jnp.bfloat16)
        items_wide = group_items.astype(jnp.float32)
        users_wide = user_vecs.astype(jnp.float32)
        columns = jnp.arange(group_users, dtype=jnp.int32)

        def block_step(accum, block_no):
            first_row = (block_no * row_block).astype(jnp.int32)
            user_block = lax.dynamic_slice_in_dim(users_wide, first_row, row_block, 0)
            weight_block = lax.dynamic_slice_in_dim(weights, first_row, row_block, 0)
            target_block = lax.dynamic_slice_in_dim(targets, first_row, row_block, 0)
            scores = jnp.dot(user_block, items_wide.T)
            row_max = jnp.max(scores, axis=1, keepdims=True)
            log_total = row_max + jnp.log(jnp.sum(jnp.exp(scores - row_max), axis=1, keepdims=True))
            chosen = (columns[None, :] == target_block[:, None]).astype(jnp.float32)
            dscore = (weight_block[:, None] * (jnp.exp(scores - log_total) - chosen)).astype(jnp.bfloat16)
            dscore_wide = dscore.astype(jnp.float32)
            grad_block = jnp.dot(dscore_wide, items_wide)
            accum = accum + jnp.dot(dscore_wide.T, user_block)
            return accum, grad_block

        grad_item, grad_blocks = lax.scan(block_step, jnp.zeros((group_users, D), jnp.float32),
                                          jnp.arange(num_blocks, dtype=jnp.int32))
        grad_user = grad_blocks.reshape(group_users, D).astype(jnp.bfloat16)
        d_second = jnp.dot(hidden.T, grad_user, preferred_element_type=jnp.float32)
        back_grad = jnp.dot(grad_user, w_second.T, preferred_element_type=jnp.float32)
        sigmoid_pre = jax.nn.sigmoid(pre_act)
        grad_pre = (back_grad * sigmoid_pre * (1.0 + pre_act * (1.0 - sigmoid_pre))).astype(jnp.bfloat16)
        d_first = jnp.dot(features.T, grad_pre, preferred_element_type=jnp.float32)
        return grad_item, d_first, d_second

    grad_item, d_first, d_second = lax.map(one_group, (user_features, item_embed, example_weight, positive))
    grad_first = jnp.sum(d_first, axis=0)
    grad_second = jnp.sum(d_second, axis=0)
    table_ids = (item_owner[:, :, 0] * ITEMS_DEV + item_row).astype(jnp.int32)
    grad_table = jax.ops.segment_sum(grad_item.reshape(-1, D), table_ids.reshape(-1),
                                     num_segments=ITEMS_DEV * N_ROWS)
    return grad_first, grad_second, grad_table
```

```python
import functools
import jax
import jax.numpy as jnp
from jax import lax
from jax.experimental import pallas as pl
from jax.experimental.pallas import tpu as pltpu
from jax.sharding import PartitionSpec as P

ITEMS_DEV = 4096
F32 = jnp.float32
BF16 = jnp.bfloat16
MESH = pl.DeviceIdType.MESH


def mm(left, right, ld, rd):
    return lax.dot_general(left, right, (((ld,), (rd,)), ((), ())), preferred_element_type=F32)


def kernel(
    n, ng, lows,
    feat, w1, w2, items, stats_in,
    table, g_first, g_second,
    items_g, users_g, gat, sc, pre_buf, hid_buf, gu, gi, gt, acc,
    stats_out, stats_g, ids_in, ids_g,
    dgrad, s1_recv, s2_send, s2_recv, s3_send, s3_recv, q_buf, fin,
    ring_s, ring_r, st_s, st_r, id_s, id_r, gt_s, gt_r,
    d1_s, d1_r, d2_s, d2_r, d3_s, d3_r, d4_s, d4_r,
):
    me = lax.axis_index("rows")
    grp = lax.axis_index("grp")
    m = items.shape[0]
    half = m // 2
    full = n // 2 - 1
    cols = table.shape[0]
    span = ITEMS_DEV // lows

    def at_pos(p):
        p = lax.rem(p + 2 * n, n)
        return jnp.where(p < n // 2, 2 * p, 2 * (n - 1 - p) + 1)

    odd = lax.rem(me, 2)
    pos = jnp.where(odd == 0, me // 2, n - 1 - me // 2)
    right, left = at_pos(pos + 1), at_pos(pos - 1)

    def row_peer(k):
        return lax.rem(me + k, n)

    def grp_peer(k):
        return lax.rem(grp + k, ng)

    def remote(src, dst, ss, rs, rows=None, grps=None):
        return pltpu.make_async_remote_copy(
            src_ref=src, dst_ref=dst, send_sem=ss, recv_sem=rs,
            device_id=(me if rows is None else rows, grp if grps is None else grps),
            device_id_type=MESH,
        )

    def hop(which, buf, h, d, c, first=None):
        origin = at_pos(pos - h) if d == 0 else at_pos(pos + h)
        size = buf.shape[1] // 2
        dst = buf.at[origin, pl.ds(c * size, size)]
        src = dst if first is None else first.at[pl.ds(c * size, size)]
        return remote(
            src, dst, ring_s.at[which, d, h, c], ring_r.at[which, d, h, c],
            rows=right if d == 0 else left,
        )

    def arrive(which, buf, h, d, c):
        origin = at_pos(pos - h - 1) if d == 0 else at_pos(pos + h + 1)
        size = buf.shape[1] // 2
        dst = buf.at[origin, pl.ds(c * size, size)]
        remote(
            dst, dst, ring_s.at[which, d, h, c], ring_r.at[which, d, h, c],
            rows=right if d == 0 else left,
        ).wait_recv()
        return origin

    def ring_start(which, buf, first=None):
        for c in range(2):
            for d in range(2):
                if full > 0 or c == d:
                    hop(which, buf, 0, d, c, first).start()

    def ring_full(which, buf, h):
        for c in range(2):
            for d in range(2):
                arrive(which, buf, h, d, c)
                hop(which, buf, h + 1, d, c).start()

    def ring_turn(which, buf, h):
        for d in range(2):
            arrive(which, buf, h, d, d)
            hop(which, buf, h + 1, d, d).start()
        for d in range(2):
            arrive(which, buf, h, d, 1 - d)

    def ring_end(which, buf):
        for d in range(2):
            arrive(which, buf, full, d, d)

    def ring_sent(which, buf, first=None):
        for d in range(2):
            for c in range(2):
                for h in range(full + 1):
                    if h < full or c == d:
                        hop(which, buf, h, d, c, first if h == 0 else None).wait_send()

    def behind(h):
        return at_pos(pos - h - 1), at_pos(pos + h + 1)

    far = at_pos(pos + n // 2)

    barrier = pltpu.get_barrier_semaphore()
    for k in range(1, n):
        pl.semaphore_signal(barrier, inc=1, device_id=(row_peer(k), grp), device_id_type=MESH)
    for k in range(1, ng):
        pl.semaphore_signal(barrier, inc=1, device_id=(me, grp_peer(k)), device_id_type=MESH)

    pre = mm(feat[...], w1[...], 1, 0)
    pre_buf[...] = pre
    hidden = (pre * jax.nn.sigmoid(pre)).astype(BF16)
    hid_buf[...] = hidden
    own_users = mm(hidden, w2[...], 1, 0).astype(BF16)
    users_g[me] = own_users
    items_g[me] = items[...]
    acc[...] = jnp.zeros_like(acc)

    pl.semaphore_wait(barrier, n - 1 + ng - 1)
    ring_start(0, items_g, items)

    def id_copy(k):
        return remote(stats_in, ids_in.at[grp], id_s.at[k - 1], id_r.at[k - 1], grps=grp_peer(k))

    for k in range(1, ng):
        id_copy(k).start()

    def score(b, top):
        s = mm(items_g[b], users_g[me], 1, 1)
        sc[b] = s
        return jnp.maximum(top, jnp.max(s, axis=0, keepdims=True))

    top = score(me, jnp.full((1, m), -jnp.inf, F32))

    def step_items(h, top):
        ring_full(0, items_g, h)
        for b in behind(h):
            top = score(b, top)
        return top

    if full > 0:
        top = lax.fori_loop(0, full - 1, step_items, top)
        ring_turn(0, items_g, full - 1)
    ring_start(1, users_g)
    if full > 0:
        for b in behind(full - 1):
            top = score(b, top)
    ring_end(0, items_g)
    top = score(far, top)

    weight = stats_in[1:2, :]
    target = stats_in[2:3, :].astype(jnp.int32)

    total = lax.fori_loop(
        0, n, lambda b, t: t + jnp.sum(jnp.exp(sc[b] - top), axis=0, keepdims=True),
        jnp.zeros((1, m), F32),
    )
    log_total = top + jnp.log(total)

    ids_in[grp] = stats_in[...]
    for k in range(1, ng):
        src = lax.rem(grp + ng - k, ng)
        remote(
            stats_in, ids_in.at[src], id_s.at[k - 1], id_r.at[k - 1], grps=grp_peer(k)
        ).wait_recv()
    stats_out[0:1, :] = log_total
    stats_out[1:2, :] = weight
    stats_out[2:3, :] = stats_in[2:3, :]
    for q in range(ng):
        stats_out[3 + q : 4 + q, :] = ids_in[q, 3:4, :]
    for q in range(3 + ng, stats_out.shape[0]):
        stats_out[q : q + 1, :] = jnp.zeros((1, m), F32)

    def stat_copy(k, slot):
        return remote(stats_out, stats_g.at[slot], st_s.at[k - 1], st_r.at[k - 1], rows=row_peer(k))

    for k in range(1, n):
        stat_copy(k, me).start()
    stats_g[me] = stats_out[...]
    if full > 1:
        ring_full(1, users_g, 0)

    gu[...] = jnp.zeros_like(gu)

    def back_user(b, carry):
        rows_at = b * m + lax.broadcasted_iota(jnp.int32, (m, m), 0)
        hit = (rows_at == target).astype(F32)
        ds = (weight * (jnp.exp(sc[b] - log_total) - hit)).astype(BF16)
        gu[...] += mm(ds, items_g[b], 0, 0)
        return carry

    lax.fori_loop(0, n, back_user, 0)
    grad_user = gu[...].astype(BF16)
    back = mm(grad_user, w2[...], 1, 1)
    pre = pre_buf[...]
    sig = jax.nn.sigmoid(pre)
    grad_pre = (back * sig * (1.0 + pre * (1.0 - sig))).astype(BF16)
    dh = w1.shape[0]
    dgrad[0:dh, :] = mm(feat[...], grad_pre, 0, 0)
    dgrad[dh:, :] = mm(hid_buf[...], grad_user, 0, 0)
    quarter = dgrad.shape[0] // ng

    def d1_copy(k):
        return remote(
            dgrad.at[pl.ds(pl.multiple_of(grp_peer(k) * quarter, quarter), quarter)],
            s1_recv.at[k - 1], d1_s.at[k - 1], d1_r.at[k - 1], grps=grp_peer(k),
        )

    for k in range(1, ng):
        d1_copy(k).start()

    for k in range(1, n):
        stat_copy(k, lax.rem(me + n - k, n)).wait_recv()
    own_rows = me * m + lax.broadcasted_iota(jnp.int32, (m, m), 0)
    gi[...] = jnp.zeros_like(gi)

    def back_item(b):
        st = stats_g[b]
        s = mm(items[...], users_g[b], 1, 1)
        hit = (own_rows == st[2:3, :].astype(jnp.int32)).astype(F32)
        ds = (st[1:2, :] * (jnp.exp(s - st[0:1, :]) - hit)).astype(BF16)
        gi[...] += mm(ds, users_g[b], 1, 0)

    back_item(me)
    if full > 1:
        for b in behind(0):
            back_item(b)

    def step_users(h, carry):
        ring_full(1, users_g, h)
        for b in behind(h):
            back_item(b)
        return carry

    if full > 0:
        if full > 2:
            lax.fori_loop(1, full - 1, step_users, 0)
        ring_turn(1, users_g, full - 1)
        for b in behind(full - 1):
            back_item(b)

    piece = quarter // n
    for k in range(1, ng):
        d1_copy(k).wait_recv()
    part = dgrad[pl.ds(pl.multiple_of(grp * quarter, quarter), quarter), :]
    for k in range(1, ng):
        part = part + s1_recv[k - 1]
    for q in range(n):
        s2_send[q] = part[q * piece : (q + 1) * piece, :]

    def d2_copy(k):
        return remote(
            s2_send.at[row_peer(k)], s2_recv.at[k - 1], d2_s.at[k - 1], d2_r.at[k - 1],
            rows=row_peer(k),
        )

    for k in range(1, n):
        d2_copy(k).start()

    ring_end(1, users_g)
    back_item(far)
    turned = jnp.transpose(gi[...]).astype(BF16)
    for q in range(ng):
        gt[q] = turned[q * cols : (q + 1) * cols, :]

    def gt_copy(k, slot):
        return remote(
            gt.at[grp_peer(k)], gat.at[me, slot], gt_s.at[k - 1], gt_r.at[k - 1], grps=grp_peer(k)
        )

    for k in range(1, ng):
        gt_copy(k, grp).start()
    gat[me, grp] = gt[grp]

    for k in range(1, n):
        d2_copy(k).wait_recv()
    one = s2_send[me]
    for k in range(1, n):
        one = one + s2_recv[k - 1]
    s3_send[...] = one
    s3_recv[me] = one

    for k in range(1, ng):
        gt_copy(k, lax.rem(grp + ng - k, ng)).wait_recv()
    ring_start(2, gat)

    def d3_copy(k, slot):
        return remote(s3_send, s3_recv.at[slot], d3_s.at[k - 1], d3_r.at[k - 1], rows=row_peer(k))

    for k in range(1, n):
        d3_copy(k, me).start()

    def place(b):
        ids = stats_g[b, 3 : 3 + ng, :].astype(jnp.int32) - me * ITEMS_DEV
        for q in range(ng):
            own = ids[q : q + 1, :]
            own = jnp.where((own >= 0) & (own < ITEMS_DEV), own, -1)
            low = own // span
            high = jnp.where(own < 0, -1, own - low * span)
            pick = (lax.broadcasted_iota(jnp.int32, (span, m), 0) == high).astype(F32).astype(BF16)
            values = gat[b, q]
            zero = jnp.zeros_like(values)
            lifted = jnp.concatenate(
                [
                    jnp.where(jnp.broadcast_to(low, values.shape) == v, values, zero)
                    for v in range(lows)
                ],
                axis=0,
            )
            acc[...] += mm(lifted, pick, 1, 1)

    place(me)

    def step_table(h, carry):
        ring_full(2, gat, h)
        for b in behind(h):
            place(b)
        return carry

    if full > 0:
        lax.fori_loop(0, full - 1, step_table, 0)
        ring_turn(2, gat, full - 1)

    for k in range(1, n):
        d3_copy(k, lax.rem(me + n - k, n)).wait_recv()
    q_buf[...] = jnp.concatenate([s3_recv[q] for q in range(n)], axis=0).astype(BF16)
    fin[grp] = q_buf[...]

    def d4_copy(k, slot):
        return remote(q_buf, fin.at[slot], d4_s.at[k - 1], d4_r.at[k - 1], grps=grp_peer(k))

    for k in range(1, ng):
        d4_copy(k, grp).start()

    if full > 0:
        for b in behind(full - 1):
            place(b)
    ring_end(2, gat)
    place(far)
    for v in range(lows):
        table[:, v * span : (v + 1) * span] = acc[v * cols : (v + 1) * cols, :]

    for k in range(1, ng):
        d4_copy(k, lax.rem(grp + ng - k, ng)).wait_recv()
    for q in range(ng):
        first = q * quarter
        out, base = (g_first, first) if first < dh else (g_second, first - dh)
        out[base : base + quarter, :] = fin[q].astype(F32)

    ring_sent(0, items_g, items)
    ring_sent(1, users_g)
    ring_sent(2, gat)
    for k in range(1, n):
        stat_copy(k, me).wait_send()
        d2_copy(k).wait_send()
        d3_copy(k, me).wait_send()
    for k in range(1, ng):
        id_copy(k).wait_send()
        d1_copy(k).wait_send()
        gt_copy(k, grp).wait_send()
        d4_copy(k, grp).wait_send()


def body(
    n, ng,
    user_features, w_first, w_second, item_embed, example_weight, positive, item_owner, item_row
):
    m, d = item_embed.shape[1], item_embed.shape[2]
    dh = w_first.shape[0]
    cols = d // ng
    lows = 8
    span = ITEMS_DEV // lows
    ids = item_owner[:, :, 0] * ITEMS_DEV + item_row
    stats_in = jnp.concatenate(
        [
            jnp.zeros((1, m), F32), example_weight, positive.astype(F32), ids.astype(F32),
            jnp.zeros((4, m), F32),
        ],
        axis=0,
    )
    srows = -(-(3 + ng) // 8) * 8
    quarter = 2 * dh // ng
    piece = quarter // n
    hops = n // 2
    vmem = pl.BlockSpec(memory_space=pltpu.VMEM)
    sem = pltpu.SemaphoreType.DMA
    table, g_first, g_second = pl.pallas_call(
        functools.partial(kernel, n, ng, lows),
        out_shape=(
            jax.ShapeDtypeStruct((cols, ITEMS_DEV), F32),
            jax.ShapeDtypeStruct(w_first.shape, F32),
            jax.ShapeDtypeStruct(w_second.shape, F32),
        ),
        in_specs=[vmem] * 5,
        out_specs=(vmem,) * 3,
        scratch_shapes=[
            pltpu.VMEM((n, m, d), BF16),
            pltpu.VMEM((n, m, d), BF16),
            pltpu.VMEM((n, ng, cols, m), BF16),
            pltpu.VMEM((n, m, m), F32),
            pltpu.VMEM((m, dh), F32),
            pltpu.VMEM((m, dh), BF16),
            pltpu.VMEM((m, d), F32),
            pltpu.VMEM((m, d), F32),
            pltpu.VMEM((ng, cols, m), BF16),
            pltpu.VMEM((lows * cols, span), F32),
            pltpu.VMEM((srows, m), F32),
            pltpu.VMEM((n, srows, m), F32),
            pltpu.VMEM((ng, 8, m), F32),
            pltpu.VMEM((8, m), F32),
            pltpu.VMEM((2 * dh, d), F32),
            pltpu.VMEM((ng - 1, quarter, d), F32),
            pltpu.VMEM((n, piece, d), F32),
            pltpu.VMEM((n - 1, piece, d), F32),
            pltpu.VMEM((piece, d), F32),
            pltpu.VMEM((n, piece, d), F32),
            pltpu.VMEM((quarter, d), BF16),
            pltpu.VMEM((ng, quarter, d), BF16),
            sem((3, 2, hops, 2)), sem((3, 2, hops, 2)),
            sem((n - 1,)), sem((n - 1,)),
            sem((ng - 1,)), sem((ng - 1,)),
            sem((ng - 1,)), sem((ng - 1,)),
            sem((ng - 1,)), sem((ng - 1,)),
            sem((n - 1,)), sem((n - 1,)),
            sem((n - 1,)), sem((n - 1,)),
            sem((ng - 1,)), sem((ng - 1,)),
        ],
        compiler_params=pltpu.CompilerParams(
            collective_id=0, has_side_effects=True, vmem_limit_bytes=60 * 1024 * 1024
        ),
    )(user_features[0], w_first, w_second, item_embed[0], stats_in)
    return g_first, g_second, jnp.transpose(table)


def solution(mesh):
    placed = (
        P("grp", "rows", None),
        P(),
        P(),
        P("grp", "rows", None),
        P("grp", "rows"),
        P("grp", "rows"),
        P("grp", "rows", None),
        P("grp", "rows"),
    )
    return jax.shard_map(
        functools.partial(body, mesh.shape["rows"], mesh.shape["grp"]),
        mesh=mesh, in_specs=placed, out_specs=(P(), P(), P("rows", "grp")), check_vma=False
    )
```

```python
import functools
import jax
import jax.numpy as jnp
from jax import lax
from jax.experimental import pallas as pl
from jax.experimental.pallas import tpu as pltpu
from jax.sharding import PartitionSpec as P

ITEMS_DEV = 4096
F32 = jnp.float32
BF16 = jnp.bfloat16
MESH = pl.DeviceIdType.MESH
CHUNKS = 4


def mm(left, right, ld, rd):
    return lax.dot_general(left, right, (((ld,), (rd,)), ((), ())), preferred_element_type=F32)


def kernel(
    n, ng, lows,
    feat, w1, w2, items, weight_in, target_in, owner_in, row_in,
    table, g_both,
    items_g, users_g, gat, sc, pre_buf, hid_buf, gu, gi, gt, acc,
    stats_out, stats_g, ids_in, stats_in,
    dgrad, s1_recv, s2_send, s2_recv, s3_send, s3_recv, q_buf, fin,
    ring_s, ring_r, st_s, st_r, id_s, id_r, gt_s, gt_r,
    d1_s, d1_r, d2_s, d2_r, d3_s, d3_r, d4_s, d4_r,
):
    me = lax.axis_index("rows")
    grp = lax.axis_index("grp")
    m = items.shape[0]
    lasts = (range(CHUNKS // 2), range(CHUNKS // 2, CHUNKS))
    full = n // 2 - 1
    cols = table.shape[0]
    span = ITEMS_DEV // lows

    def at_pos(p):
        p = lax.rem(p + 2 * n, n)
        return jnp.where(p < n // 2, 2 * p, 2 * (n - 1 - p) + 1)

    odd = lax.rem(me, 2)
    pos = jnp.where(odd == 0, me // 2, n - 1 - me // 2)
    right, left = at_pos(pos + 1), at_pos(pos - 1)

    def row_peer(k):
        return lax.rem(me + k, n)

    def grp_peer(k):
        return lax.rem(grp + k, ng)

    def remote(src, dst, ss, rs, rows=None, grps=None):
        return pltpu.make_async_remote_copy(
            src_ref=src, dst_ref=dst, send_sem=ss, recv_sem=rs,
            device_id=(me if rows is None else rows, grp if grps is None else grps),
            device_id_type=MESH,
        )

    def hop(which, buf, h, d, c, first=None):
        origin = at_pos(pos - h) if d == 0 else at_pos(pos + h)
        size = buf.shape[1] // CHUNKS
        dst = buf.at[origin, pl.ds(c * size, size)]
        src = dst if first is None else first.at[pl.ds(c * size, size)]
        return remote(
            src, dst, ring_s.at[which, d, h, c], ring_r.at[which, d, h, c],
            rows=right if d == 0 else left,
        )

    def arrive(which, buf, h, d, c):
        origin = at_pos(pos - h - 1) if d == 0 else at_pos(pos + h + 1)
        size = buf.shape[1] // CHUNKS
        dst = buf.at[origin, pl.ds(c * size, size)]
        remote(
            dst, dst, ring_s.at[which, d, h, c], ring_r.at[which, d, h, c],
            rows=right if d == 0 else left,
        ).wait_recv()
        return origin

    def ring_start(which, buf, first=None):
        for c in range(CHUNKS):
            for d in range(2):
                if full > 0 or c in lasts[d]:
                    hop(which, buf, 0, d, c, first).start()

    def ring_full(which, buf, h):
        for c in range(CHUNKS):
            for d in range(2):
                arrive(which, buf, h, d, c)
                hop(which, buf, h + 1, d, c).start()

    def ring_turn(which, buf, h):
        for c in range(CHUNKS):
            for d in range(2):
                arrive(which, buf, h, d, c)
                if c in lasts[d]:
                    hop(which, buf, h + 1, d, c).start()

    def ring_end(which, buf):
        for d in range(2):
            for c in lasts[d]:
                arrive(which, buf, full, d, c)

    def ring_sent(which, buf, first=None):
        for d in range(2):
            for c in range(CHUNKS):
                for h in range(full + 1):
                    if h < full or c in lasts[d]:
                        hop(which, buf, h, d, c, first if h == 0 else None).wait_send()

    def behind(h):
        return at_pos(pos - h - 1), at_pos(pos + h + 1)

    far = at_pos(pos + n // 2)

    barrier = pltpu.get_barrier_semaphore()
    for k in range(1, n):
        pl.semaphore_signal(barrier, inc=1, device_id=(row_peer(k), grp), device_id_type=MESH)
    for k in range(1, ng):
        pl.semaphore_signal(barrier, inc=1, device_id=(me, grp_peer(k)), device_id_type=MESH)

    pre = mm(feat[...], w1[...], 1, 0)
    pre_buf[...] = pre
    hidden = (pre * jax.nn.sigmoid(pre)).astype(BF16)
    hid_buf[...] = hidden
    own_users = mm(hidden, w2[...], 1, 0).astype(BF16)
    users_g[me] = own_users
    items_g[me] = items[...]
    acc[...] = jnp.zeros_like(acc)
    stats_in[...] = jnp.zeros_like(stats_in)
    stats_in[1:2, :] = weight_in[...]
    stats_in[2:3, :] = target_in[...].astype(F32)
    stats_in[3:4, :] = (owner_in[...] * ITEMS_DEV + row_in[...]).astype(F32)

    pl.semaphore_wait(barrier, n - 1 + ng - 1)
    ring_start(0, items_g, items)
    ring_start(1, users_g)

    def id_copy(k):
        return remote(stats_in, ids_in.at[grp], id_s.at[k - 1], id_r.at[k - 1], grps=grp_peer(k))

    for k in range(1, ng):
        id_copy(k).start()

    def score(b, top):
        s = mm(items_g[b], users_g[me], 1, 1)
        sc[b] = s
        return jnp.maximum(top, jnp.max(s, axis=0, keepdims=True))

    top = score(me, jnp.full((1, m), -jnp.inf, F32))

    def step_items(h, top):
        ring_full(0, items_g, h)
        for b in behind(h):
            top = score(b, top)
        return top

    if full > 0:
        top = lax.fori_loop(0, full - 1, step_items, top)
    if full > 0:
        ring_turn(0, items_g, full - 1)
    if full > 0:
        for b in behind(full - 1):
            top = score(b, top)
    ring_end(0, items_g)
    if full > 1:
        ring_full(1, users_g, 0)
    top = score(far, top)

    weight = stats_in[1:2, :]
    target = target_in[...]

    total = lax.fori_loop(
        0, n, lambda b, t: t + jnp.sum(jnp.exp(sc[b] - top), axis=0, keepdims=True),
        jnp.zeros((1, m), F32),
    )
    log_total = top + jnp.log(total)

    ids_in[grp] = stats_in[...]
    for k in range(1, ng):
        src = lax.rem(grp + ng - k, ng)
        remote(
            stats_in, ids_in.at[src], id_s.at[k - 1], id_r.at[k - 1], grps=grp_peer(k)
        ).wait_recv()
    stats_out[0:1, :] = log_total
    stats_out[1:2, :] = weight
    stats_out[2:3, :] = stats_in[2:3, :]
    for q in range(ng):
        stats_out[3 + q : 4 + q, :] = ids_in[q, 3:4, :]
    for q in range(3 + ng, stats_out.shape[0]):
        stats_out[q : q + 1, :] = jnp.zeros((1, m), F32)

    def stat_copy(k, slot):
        return remote(stats_out, stats_g.at[slot], st_s.at[k - 1], st_r.at[k - 1], rows=row_peer(k))

    for k in range(1, n):
        stat_copy(k, me).start()
    stats_g[me] = stats_out[...]

    gu[...] = jnp.zeros_like(gu)

    def back_user(b, carry):
        rows_at = b * m + lax.broadcasted_iota(jnp.int32, (m, m), 0)
        hit = (rows_at == target).astype(F32)
        ds = (weight * (jnp.exp(sc[b] - log_total) - hit)).astype(BF16)
        gu[...] += mm(ds, items_g[b], 0, 0)
        return carry

    lax.fori_loop(0, n, back_user, 0)

    def step_users(h, carry):
        ring_full(1, users_g, h)
        return carry

    if full > 2:
        lax.fori_loop(1, full - 1, step_users, 0)
    grad_user = gu[...].astype(BF16)
    back = mm(grad_user, w2[...], 1, 1)
    pre = pre_buf[...]
    sig = jax.nn.sigmoid(pre)
    grad_pre = (back * sig * (1.0 + pre * (1.0 - sig))).astype(BF16)
    dh = w1.shape[0]
    dgrad[0:dh, :] = mm(feat[...], grad_pre, 0, 0)
    dgrad[dh:, :] = mm(hid_buf[...], grad_user, 0, 0)
    quarter = dgrad.shape[0] // ng

    def d1_copy(k):
        return remote(
            dgrad.at[pl.ds(pl.multiple_of(grp_peer(k) * quarter, quarter), quarter)],
            s1_recv.at[k - 1], d1_s.at[k - 1], d1_r.at[k - 1], grps=grp_peer(k),
        )

    for k in range(1, ng):
        d1_copy(k).start()
    if full > 0:
        ring_turn(1, users_g, full - 1)

    for k in range(1, n):
        stat_copy(k, lax.rem(me + n - k, n)).wait_recv()
    own_rows = me * m + lax.broadcasted_iota(jnp.int32, (m, m), 0)
    gi[...] = jnp.zeros_like(gi)

    def back_item(b):
        st = stats_g[b]
        s = mm(items[...], users_g[b], 1, 1)
        hit = (own_rows == st[2:3, :].astype(jnp.int32)).astype(F32)
        ds = (st[1:2, :] * (jnp.exp(s - st[0:1, :]) - hit)).astype(BF16)
        gi[...] += mm(ds, users_g[b], 1, 0)

    back_item(me)

    def step_items_back(h, carry):
        for b in behind(h):
            back_item(b)
        return carry

    lax.fori_loop(0, full, step_items_back, 0)

    piece = quarter // n
    for k in range(1, ng):
        d1_copy(k).wait_recv()
    part = dgrad[pl.ds(pl.multiple_of(grp * quarter, quarter), quarter), :]
    for k in range(1, ng):
        part = part + s1_recv[k - 1]
    for q in range(n):
        s2_send[q] = part[q * piece : (q + 1) * piece, :]

    def d2_copy(k):
        return remote(
            s2_send.at[row_peer(k)], s2_recv.at[k - 1], d2_s.at[k - 1], d2_r.at[k - 1],
            rows=row_peer(k),
        )

    for k in range(1, n):
        d2_copy(k).start()

    ring_end(1, users_g)
    back_item(far)
    turned = jnp.transpose(gi[...]).astype(BF16)
    for q in range(ng):
        gt[q] = turned[q * cols : (q + 1) * cols, :]

    def gt_copy(k, slot):
        return remote(
            gt.at[grp_peer(k)], gat.at[me, slot], gt_s.at[k - 1], gt_r.at[k - 1], grps=grp_peer(k)
        )

    for k in range(1, ng):
        gt_copy(k, grp).start()
    gat[me, grp] = gt[grp]

    for k in range(1, n):
        d2_copy(k).wait_recv()
    one = s2_send[me]
    for k in range(1, n):
        one = one + s2_recv[k - 1]
    s3_send[...] = one.astype(BF16)
    s3_recv[me] = one.astype(BF16)

    for k in range(1, ng):
        gt_copy(k, lax.rem(grp + ng - k, ng)).wait_recv()
    ring_start(2, gat)

    def d3_copy(k, slot):
        return remote(s3_send, s3_recv.at[slot], d3_s.at[k - 1], d3_r.at[k - 1], rows=row_peer(k))

    for k in range(1, n):
        d3_copy(k, me).start()

    def place(b):
        ids = stats_g[b, 3 : 3 + ng, :].astype(jnp.int32) - me * ITEMS_DEV
        for q in range(ng):
            own = ids[q : q + 1, :]
            own = jnp.where((own >= 0) & (own < ITEMS_DEV), own, -1)
            low = own // span
            high = jnp.where(own < 0, -1, own - low * span)
            pick = (lax.broadcasted_iota(jnp.int32, (span, m), 0) == high).astype(F32).astype(BF16)
            values = gat[b, q]
            zero = jnp.zeros_like(values)
            lifted = jnp.concatenate(
                [
                    jnp.where(jnp.broadcast_to(low, values.shape) == v, values, zero)
                    for v in range(lows)
                ],
                axis=0,
            )
            acc[...] += mm(lifted, pick, 1, 1)

    place(me)

    def step_table(h, carry):
        ring_full(2, gat, h)
        for b in behind(h):
            place(b)
        return carry

    if full > 0:
        lax.fori_loop(0, full - 1, step_table, 0)
        ring_turn(2, gat, full - 1)

    for k in range(1, n):
        d3_copy(k, lax.rem(me + n - k, n)).wait_recv()
    q_buf[...] = jnp.concatenate([s3_recv[q] for q in range(n)], axis=0)
    fin[grp] = q_buf[...]

    def d4_copy(k, slot):
        return remote(q_buf, fin.at[slot], d4_s.at[k - 1], d4_r.at[k - 1], grps=grp_peer(k))

    for k in range(1, ng):
        d4_copy(k, grp).start()

    if full > 0:
        for b in behind(full - 1):
            place(b)
    ring_end(2, gat)
    place(far)
    for v in range(lows):
        table[:, v * span : (v + 1) * span] = acc[v * cols : (v + 1) * cols, :]

    for k in range(1, ng):
        d4_copy(k, lax.rem(grp + ng - k, ng)).wait_recv()
    for q in range(ng):
        g_both[q * quarter : (q + 1) * quarter, :] = fin[q]

    ring_sent(0, items_g, items)
    ring_sent(1, users_g)
    ring_sent(2, gat)
    for k in range(1, n):
        stat_copy(k, me).wait_send()
        d2_copy(k).wait_send()
        d3_copy(k, me).wait_send()
    for k in range(1, ng):
        id_copy(k).wait_send()
        d1_copy(k).wait_send()
        gt_copy(k, grp).wait_send()
        d4_copy(k, grp).wait_send()


def body(
    n, ng,
    user_features, w_first, w_second, item_embed, example_weight, positive, item_owner, item_row
):
    m, d = item_embed.shape[1], item_embed.shape[2]
    dh = w_first.shape[0]
    cols = d // ng
    lows = 8
    span = ITEMS_DEV // lows
    srows = -(-(3 + ng) // 8) * 8
    quarter = 2 * dh // ng
    piece = quarter // n
    hops = n // 2
    vmem = pl.BlockSpec(memory_space=pltpu.VMEM)
    sem = pltpu.SemaphoreType.DMA
    table, g_both = pl.pallas_call(
        functools.partial(kernel, n, ng, lows),
        out_shape=(
            jax.ShapeDtypeStruct((cols, ITEMS_DEV), F32),
            jax.ShapeDtypeStruct((2 * dh, d), BF16),
        ),
        in_specs=[vmem] * 8,
        out_specs=(vmem,) * 2,
        scratch_shapes=[
            pltpu.VMEM((n, m, d), BF16),
            pltpu.VMEM((n, m, d), BF16),
            pltpu.VMEM((n, ng, cols, m), BF16),
            pltpu.VMEM((n, m, m), F32),
            pltpu.VMEM((m, dh), F32),
            pltpu.VMEM((m, dh), BF16),
            pltpu.VMEM((m, d), F32),
            pltpu.VMEM((m, d), F32),
            pltpu.VMEM((ng, cols, m), BF16),
            pltpu.VMEM((lows * cols, span), F32),
            pltpu.VMEM((srows, m), F32),
            pltpu.VMEM((n, srows, m), F32),
            pltpu.VMEM((ng, 8, m), F32),
            pltpu.VMEM((8, m), F32),
            pltpu.VMEM((2 * dh, d), F32),
            pltpu.VMEM((ng - 1, quarter, d), F32),
            pltpu.VMEM((n, piece, d), F32),
            pltpu.VMEM((n - 1, piece, d), F32),
            pltpu.VMEM((piece, d), BF16),
            pltpu.VMEM((n, piece, d), BF16),
            pltpu.VMEM((quarter, d), BF16),
            pltpu.VMEM((ng, quarter, d), BF16),
            sem((3, 2, hops, CHUNKS)), sem((3, 2, hops, CHUNKS)),
            sem((n - 1,)), sem((n - 1,)),
            sem((ng - 1,)), sem((ng - 1,)),
            sem((ng - 1,)), sem((ng - 1,)),
            sem((ng - 1,)), sem((ng - 1,)),
            sem((n - 1,)), sem((n - 1,)),
            sem((n - 1,)), sem((n - 1,)),
            sem((ng - 1,)), sem((ng - 1,)),
        ],
        compiler_params=pltpu.CompilerParams(
            collective_id=0, has_side_effects=True, vmem_limit_bytes=60 * 1024 * 1024
        ),
    )(
        user_features[0], w_first, w_second, item_embed[0],
        example_weight, positive, item_owner.reshape(1, m), item_row,
    )
    return g_both[:dh].astype(F32), g_both[dh:].astype(F32), jnp.transpose(table)


def solution(mesh):
    placed = (
        P("grp", "rows", None),
        P(),
        P(),
        P("grp", "rows", None),
        P("grp", "rows"),
        P("grp", "rows"),
        P("grp", "rows", None),
        P("grp", "rows"),
    )
    return jax.shard_map(
        functools.partial(body, mesh.shape["rows"], mesh.shape["grp"]),
        mesh=mesh, in_specs=placed, out_specs=(P(), P(), P("rows", "grp")), check_vma=False
    )
```
